8 devices in a mesh: fsdp: 4 (over z, y, x), ep: 2 (over core).
Axes of the slice: x: 2, y: 2, z: 1, core: 2. Of those that a mesh axis runs over, the one named last changes fastest.
Arguments:
- x_in: bfloat16 [2, 16384, 768], P(None, ('fsdp', 'ep'))
- dy_out: bfloat16 [2, 16384, 768], P(None, ('fsdp', 'ep'))
- expert_idx: int32 [2, 16384, 2], P(None, ('fsdp', 'ep'))
- gate_prob: float32 [2, 16384, 2], P(None, ('fsdp', 'ep'))
- w_one: bfloat16 [8, 768, 4096], P('ep', 'fsdp')
- w_two: bfloat16 [8, 4096, 768], P('ep', None, 'fsdp')
- w_three: bfloat16 [8, 768, 4096], P('ep', 'fsdp')
Outputs:
- output 1: bfloat16 [2, 16384, 768], P(None, ('fsdp', 'ep'))
- output 2: float32 [2, 16384, 2], P(None, ('fsdp', 'ep'))
- output 3: float32 [8, 768, 4096], P('ep', 'fsdp')
- output 4: float32 [8, 4096, 768], P('ep', None, 'fsdp')
- output 5: float32 [8, 768, 4096], P('ep', 'fsdp')
All inputs are finite; a program needn't handle non-finite values.
Results may differ from the reference program's by a relative error of at most 0.001.
Values are sent between devices in bfloat16 or wider.
A program may use at most 1 GiB of HBM per device.

```python
import jax
import jax.numpy as jnp
from jax import lax

D_MODEL = 768
FF_DIM = 4096
EXPERTS = 8
TOP_K = 2
TOK_DEV = 2048
SOURCES = 8
MICRO_BATCHES = 2
CAPACITY = 640

TOKENS = SOURCES * TOK_DEV
N_CHOICE = TOK_DEV * TOP_K


def draw_routing(key):
    key_hot, key_bias, key_score = jax.random.split(key, 3)
    expert_ids = jnp.arange(EXPERTS, dtype=jnp.int32)
    hot_ids = jax.random.randint(key_hot, (MICRO_BATCHES, SOURCES, 1, 1), 0, EXPERTS)
    forced = jnp.arange(TOK_DEV)[:, None] < CAPACITY
    hot_bonus = jnp.where(expert_ids == hot_ids, 1, 0) * jnp.where(forced, 4096, 512)
    source_bias = jax.random.randint(key_bias, (MICRO_BATCHES, SOURCES, 1, EXPERTS), 0, 512)
    rand_score = jax.random.randint(key_score, (MICRO_BATCHES, SOURCES, TOK_DEV, EXPERTS), 0, 1024)
    total_score = (rand_score + source_bias + hot_bonus) * EXPERTS + expert_ids
    chosen = lax.top_k(total_score, TOP_K)[1]
    return chosen.reshape(MICRO_BATCHES, TOKENS, TOP_K).astype(jnp.int32)


def setup_inputs(seed: int = 0) -> dict:
    key_list = jax.random.split(jax.random.key(seed), 7)
    x_vals = jax.random.normal(key_list[0], (MICRO_BATCHES, TOKENS, D_MODEL), jnp.float32)
    dy_vals = jax.random.normal(key_list[1], (MICRO_BATCHES, TOKENS, D_MODEL), jnp.float32)
    routing = draw_routing(key_list[2])
    gate_vals = jax.random.uniform(key_list[3], (MICRO_BATCHES, TOKENS, TOP_K), jnp.float32, 0.2, 1.0)
    w_one = jax.random.normal(key_list[4], (EXPERTS, D_MODEL, FF_DIM), jnp.float32) * D_MODEL ** -0.5
    w_two = jax.random.normal(key_list[5], (EXPERTS, FF_DIM, D_MODEL), jnp.float32) * FF_DIM ** -0.5
    w_three = jax.random.normal(key_list[6], (EXPERTS, D_MODEL, FF_DIM), jnp.float32) * D_MODEL ** -0.5
    return {'x_in': x_vals.astype(jnp.bfloat16), 'dy_out': dy_vals.astype(jnp.bfloat16), 'expert_idx': routing, 'gate_prob': gate_vals, 'w_one': w_one.astype(jnp.bfloat16), 'w_two': w_two.astype(jnp.bfloat16), 'w_three': w_three.astype(jnp.bfloat16)}


def slot_holder(ids_flat):
    one_hot = (ids_flat[:, None] == jnp.arange(EXPERTS, dtype=jnp.int32)[None, :]).astype(jnp.int32)
    position = jnp.sum((jnp.cumsum(one_hot, axis=0) - one_hot) * one_hot, axis=1)
    choice_slot = jnp.where(position < CAPACITY, ids_flat * CAPACITY + position, EXPERTS * CAPACITY)
    holder = jnp.full((EXPERTS * CAPACITY + 1,), N_CHOICE, jnp.int32)
    holder = holder.at[choice_slot].set(jnp.arange(N_CHOICE, dtype=jnp.int32))
    return holder[:EXPERTS * CAPACITY]


def expert_rows(x_rows, dy_rows, gate_rows, w_a, w_b, w_c):
    h_one = jnp.dot(x_rows, w_a, preferred_element_type=jnp.float32)
    h_three = jnp.dot(x_rows, w_c, preferred_element_type=jnp.float32)
    sigma_one = jax.nn.sigmoid(h_one)
    silu_one = h_one * sigma_one
    act_bf = (silu_one * h_three).astype(jnp.bfloat16)
    y_rows = jnp.dot(act_bf, w_b, preferred_element_type=jnp.float32)
    dg_rows = jnp.sum(dy_rows.astype(jnp.float32) * y_rows, axis=1)
    g_rows = (gate_rows[:, None] * dy_rows.astype(jnp.float32)).astype(jnp.bfloat16)
    d_act = jnp.dot(g_rows, w_b.T, preferred_element_type=jnp.float32)
    dh_three = (d_act * silu_one).astype(jnp.bfloat16)
    dh_one = (d_act * h_three * sigma_one * (1.0 + h_one * (1.0 - sigma_one))).astype(jnp.bfloat16)
    dx_rows = (jnp.dot(dh_one, w_a.T, preferred_element_type=jnp.float32) + jnp.dot(dh_three, w_c.T, preferred_element_type=jnp.float32)).astype(jnp.bfloat16)
    gw_one = jnp.dot(x_rows.T, dh_one, preferred_element_type=jnp.float32)
    gw_two = jnp.dot(act_bf.T, g_rows, preferred_element_type=jnp.float32)
    gw_three = jnp.dot(x_rows.T, dh_three, preferred_element_type=jnp.float32)
    return dx_rows, dg_rows, gw_one, gw_two, gw_three


def reference(x_in, dy_out, expert_idx, gate_prob, w_one, w_two, w_three):
    total_choices = MICRO_BATCHES * TOKENS * TOP_K
    holder = lax.map(slot_holder, expert_idx.reshape(MICRO_BATCHES * SOURCES, N_CHOICE))
    block_base = jnp.arange(MICRO_BATCHES * SOURCES, dtype=jnp.int32)[:, None] * N_CHOICE
    slot_choice = jnp.where(holder < N_CHOICE, holder + block_base, total_choices)
    slot_choice = jnp.transpose(slot_choice.reshape(MICRO_BATCHES, SOURCES, EXPERTS, CAPACITY), (2, 0, 1, 3))
    slot_choice = slot_choice.reshape(EXPERTS, MICRO_BATCHES, SOURCES * CAPACITY)
    zero_row = jnp.zeros((1, D_MODEL), x_in.dtype)
    x_flat = jnp.concatenate([x_in.reshape(MICRO_BATCHES * TOKENS, D_MODEL), zero_row], axis=0)
    dy_flat = jnp.concatenate([dy_out.reshape(MICRO_BATCHES * TOKENS, D_MODEL), zero_row], axis=0)
    gate_flat = jnp.concatenate([gate_prob.reshape(total_choices), jnp.zeros((1,), gate_prob.dtype)])

    def expert_step(scan_state, per_expert):
        dx_acc, dg_acc = scan_state
        w_a, w_b, w_c, choices = per_expert
        grad_one = jnp.zeros((D_MODEL, FF_DIM), jnp.float32)
        grad_two = jnp.zeros((FF_DIM, D_MODEL), jnp.float32)
        grad_three = jnp.zeros((D_MODEL, FF_DIM), jnp.float32)
        for mb_index in range(MICRO_BATCHES):
            pick_ids = choices[mb_index]
            tok_ids = pick_ids // TOP_K
            dx_rows, dg_rows, gw_one, gw_two, gw_three = expert_rows(x_flat[tok_ids], dy_flat[tok_ids], gate_flat[pick_ids], w_a, w_b, w_c)
            dx_acc = dx_acc.at[tok_ids].add(dx_rows.astype(jnp.float32))
            dg_acc = dg_acc.at[pick_ids].set(dg_rows)
            grad_one = grad_one + gw_one
            grad_two = grad_two + gw_two
            grad_three = grad_three + gw_three
        return (dx_acc, dg_acc), (grad_one, grad_two, grad_three)

    start_state = (jnp.zeros((MICRO_BATCHES * TOKENS + 1, D_MODEL), jnp.float32), jnp.zeros((total_choices + 1,), jnp.float32))
    end_state, grad_stack = lax.scan(expert_step, start_state, (w_one, w_two, w_three, slot_choice))
    dx_in = end_state[0][:MICRO_BATCHES * TOKENS].astype(jnp.bfloat16).reshape(MICRO_BATCHES, TOKENS, D_MODEL)
    d_gate = end_state[1][:total_choices].reshape(MICRO_BATCHES, TOKENS, TOP_K)
    return (dx_in, d_gate, grad_stack[0], grad_stack[1], grad_stack[2])
```

```python
import jax
import jax.numpy as jnp
from jax import lax
from jax.sharding import PartitionSpec as P

BLOCKS = 4
BF16 = jnp.bfloat16
F32 = jnp.float32
BOTH = ('fsdp', 'ep')


def capacity_of(tok_rows, top_k, experts):
    return 8 * ((5 * tok_rows * top_k + 32 * experts - 1) // (32 * experts))


def dot(left, right, dims):
    return lax.dot_general(left, right, ((dims[:1], dims[1:]), ((), ())), preferred_element_type=F32)


def swap(value, axes, shift, devices):
    if shift == 0:
        return value
    return lax.ppermute(value, axes, [(s, s ^ shift) for s in range(devices)])


def expert_block(x_rows, dy_rows, g_rows, w_a, w_b, w_c):
    h_one = dot(x_rows, w_a, (1, 0))
    h_three = dot(x_rows, w_c, (1, 0))
    sigma = jax.nn.sigmoid(h_one)
    silu = h_one * sigma
    act = (silu * h_three).astype(BF16)
    dg_part = jnp.sum(act.astype(F32) * dot(dy_rows, w_b, (1, 0)), axis=1)
    d_act = dot(g_rows, w_b, (1, 0))
    dh_three = (d_act * silu).astype(BF16)
    dh_one = (d_act * h_three * sigma * (1.0 + h_one * (1.0 - sigma))).astype(BF16)
    dx_part = dot(dh_one, w_a, (1, 1)) + dot(dh_three, w_c, (1, 1))
    grads = [dot(x_rows, dh_one, (0, 0)), dot(g_rows, act, (0, 0)), dot(x_rows, dh_three, (0, 0))]
    return dx_part, dg_part, grads


def solution(mesh):
    shards, ep_size = mesh.shape['fsdp'], mesh.shape['ep']
    devices = shards * ep_size
    tok_spec = P(None, BOTH, None)
    spec_edf = P('ep', 'fsdp', None)
    spec_efd = P('ep', None, 'fsdp')

    def local_step(x_in, dy_out, expert_idx, gate_prob, w_one, w_two, w_three):
        micro, tok_rows, d_model = x_in.shape
        top_k = expert_idx.shape[2]
        local_experts, d_shard, ff_dim = w_one.shape
        assert local_experts == shards
        capacity = capacity_of(tok_rows, top_k, devices)
        n_choice = tok_rows * top_k
        slots = devices * capacity
        blk = ff_dim // BLOCKS
        my_shard = lax.axis_index('fsdp')
        me = my_shard * ep_size + lax.axis_index('ep')

        def spread(pieces):
            moved = jnp.stack([swap(p, 'fsdp', k, shards) for k, p in enumerate(pieces)])
            return moved[my_shard ^ jnp.arange(shards)]

        def pick(array, index):
            return lax.dynamic_index_in_dim(array, index, 0, keepdims=False)

        ids = expert_idx.reshape(micro, n_choice)
        dest = ((ids % local_experts) * ep_size + ids // local_experts) ^ me
        one_hot = (dest[:, None, :] == jnp.arange(devices, dtype=jnp.int32)[None, :, None]).astype(jnp.int32)
        position = jnp.sum((jnp.cumsum(one_hot, axis=2) - one_hot) * one_hot, axis=1)
        choice_slot = jnp.where(position < capacity, dest * capacity + position, slots)
        holder = jnp.full((micro * (slots + 1),), n_choice, jnp.int32)
        flat_slot = choice_slot + jnp.arange(micro, dtype=jnp.int32)[:, None] * (slots + 1)
        holder = holder.at[flat_slot.reshape(-1)].set(jnp.tile(jnp.arange(n_choice, dtype=jnp.int32), micro))
        holder = holder.reshape(micro, slots + 1)[:, :slots]

        weights = jnp.stack([w_one, jnp.swapaxes(w_two, 1, 2), w_three], axis=1)
        w_blocks = []
        for b in range(BLOCKS):
            with jax.named_scope(f'w{b}'):
                piece = weights[:, :, :, b * blk:(b + 1) * blk]
                w_blk = spread([pick(piece, my_shard ^ k) for k in range(shards)])
                w_blocks.append([w_blk[:, k].reshape(d_model, blk) for k in range(3)])

        zero_row = jnp.zeros((1, 2 * d_model), x_in.dtype)
        gate_pad = jnp.concatenate([gate_prob.reshape(micro, n_choice), jnp.zeros((micro, 1), F32)], axis=1)
        dx_parts, dg_parts = [], []
        grad_sum = [None] * BLOCKS
        outs = []
        for m in range(micro):
            table = jnp.concatenate([jnp.concatenate([x_in[m], dy_out[m]], axis=1), zero_row], axis=0)
            tok_slot = (holder[m] // top_k).reshape(devices, capacity)
            gate_slot = gate_pad[m][holder[m]].reshape(devices, capacity)
            with jax.named_scope(f'tok{m}'):
                tokens = jnp.concatenate([swap(table[tok_slot[k]], BOTH, k, devices) for k in range(devices)])
                gates = jnp.concatenate([swap(gate_slot[k], BOTH, k, devices) for k in range(devices)])
            x_rows, dy_rows = tokens[:, :d_model], tokens[:, d_model:]
            g_rows = (gates[:, None] * dy_rows.astype(F32)).astype(BF16)
            dx_sum = dg_sum = None
            for b in range(BLOCKS):
                dx_part, dg_part, grads = expert_block(x_rows, dy_rows, g_rows, *w_blocks[b])
                dx_sum = dx_part if dx_sum is None else dx_sum + dx_part
                dg_sum = dg_part if dg_sum is None else dg_sum + dg_part
                grad_sum[b] = grads if m == 0 else [p + q for p, q in zip(grad_sum[b], grads)]
                if m == micro - 1:
                    send = jnp.stack([gr.reshape(shards, d_shard, blk) for gr in grad_sum[b]], axis=1)
                    with jax.named_scope(f'g{b}'):
                        outs.append(spread([pick(send, my_shard ^ k) for k in range(shards)]))
            dx_rows = dx_sum.astype(BF16).reshape(devices, capacity, d_model)
            with jax.named_scope(f'dx{m}'):
                back = jnp.concatenate([swap(dx_rows[k], BOTH, k, devices) for k in range(devices)] + [zero_row[:, :d_model]])
                dg_back = jnp.concatenate([swap(v, BOTH, k, devices) for k, v in enumerate(dg_sum.reshape(devices, capacity))] + [jnp.zeros((1,), F32)])
            picked = back[choice_slot[m]].reshape(tok_rows, top_k, d_model)
            dx_parts.append(jnp.sum(picked.astype(F32), axis=1).astype(BF16))
            dg_parts.append(dg_back[choice_slot[m]].reshape(tok_rows, top_k))
        dw_one, dw_two, dw_three = (jnp.concatenate([o[:, k] for o in outs], axis=2) for k in range(3))
        dw_two = jnp.swapaxes(dw_two, 1, 2)
        return jnp.stack(dx_parts), jnp.stack(dg_parts), dw_one, dw_two, dw_three

    return jax.shard_map(local_step, mesh=mesh, in_specs=(tok_spec, tok_spec, tok_spec, tok_spec, spec_edf, spec_efd, spec_edf), out_specs=(tok_spec, tok_spec, spec_edf, spec_efd, spec_edf), check_vma=False)
```

```python
import functools

import jax
import jax.numpy as jnp
from jax import lax
from jax.experimental import pallas as pl
from jax.experimental.pallas import tpu as pltpu
from jax.sharding import PartitionSpec as P


BLOCKS = 4
HALVES = 2
TILE = 512
CHUNK = 256
ALIGN = 16
LANES = 128
BF16 = jnp.bfloat16
F32 = jnp.float32
I32 = jnp.int32
BOTH = ('fsdp', 'ep')
ANY = pl.BlockSpec(memory_space=pl.ANY)


def capacity_of(tok_rows, top_k, experts):
    return 8 * ((5 * tok_rows * top_k + 32 * experts - 1) // (32 * experts))


def swap(value, axes, shift, devices):
    if shift == 0:
        return value
    return lax.ppermute(value, axes, [(s, s ^ shift) for s in range(devices)])


def matmul(left, right):
    return jnp.dot(left, right, preferred_element_type=F32)


def matmul_nt(left, right):
    return lax.dot_general(left, right, (((1,), (1,)), ((), ())), preferred_element_type=F32)


def params():
    return pltpu.CompilerParams(vmem_limit_bytes=60 * 2**20, dimension_semantics=None)


def pack_kernel(pieces, d_model, place, *refs):
    tok_refs, gates_ref, out_ref = refs[:pieces], refs[pieces], refs[pieces + 1]
    tok, gates, gated, in_sem, gate_sem, out_sem = refs[pieces + 2:]
    gate_copy = pltpu.make_async_copy(gates_ref, gates, gate_sem)
    gate_copy.start()
    loads = [pltpu.make_async_copy(tok_refs[k], tok.at[k], in_sem.at[k]) for k in range(pieces)]
    for load in loads:
        load.start()
    gate_copy.wait()

    def stores(k):
        first = pl.multiple_of(place[0, k], ALIGN)
        size = pl.multiple_of(place[1, k], ALIGN)
        used, rows = pl.ds(0, size), pl.ds(first, size)
        return [
            pltpu.make_async_copy(tok.at[k, used, :], out_ref.at[rows, pl.ds(0, 2 * d_model)], out_sem.at[k, 0]),
            pltpu.make_async_copy(gated.at[k, used, :], out_ref.at[rows, pl.ds(2 * d_model, d_model)], out_sem.at[k, 1]),
        ]

    for k in range(pieces):
        loads[k].wait()

        @pl.when(place[1, k] > 0)
        def _():
            for c in range(d_model // LANES):
                dy = tok[k, :, pl.ds(d_model + c * LANES, LANES)].astype(F32)
                gated[k, :, pl.ds(c * LANES, LANES)] = (gates[k] * dy).astype(BF16)
            for store in stores(k):
                store.start()

    for k in range(pieces):
        @pl.when(place[1, k] > 0)
        def _():
            for store in stores(k):
                store.wait()


def pack(place, tokens, gates, capacity, d_model):
    pieces = len(tokens)
    return pl.pallas_call(
        functools.partial(pack_kernel, pieces, d_model),
        out_shape=jax.ShapeDtypeStruct((pieces * capacity, 3 * d_model), BF16),
        in_specs=[pl.BlockSpec(memory_space=pltpu.SMEM)] + [ANY] * (pieces + 1),
        out_specs=ANY,
        scratch_shapes=[
            pltpu.VMEM((pieces, capacity, 2 * d_model), BF16),
            pltpu.VMEM((pieces, capacity, LANES), F32),
            pltpu.VMEM((pieces, capacity, d_model), BF16),
            pltpu.SemaphoreType.DMA((pieces,)),
            pltpu.SemaphoreType.DMA,
            pltpu.SemaphoreType.DMA((pieces, 2)),
        ],
        compiler_params=params(),
        cost_estimate=pl.CostEstimate(flops=10**9, bytes_accessed=40 * 2**20, transcendentals=0),
        name='pack',
    )(place, *tokens, gates)


def unpack_kernel(pieces, place, packed_ref, *refs):
    out_refs = refs[:pieces]
    rows_ref, in_sem, out_sem = refs[pieces:]
    load = pltpu.make_async_copy(packed_ref, rows_ref, in_sem)
    load.start()
    load.wait()

    def store(k):
        first = pl.multiple_of(place[0, k], ALIGN)
        size = pl.multiple_of(place[1, k], ALIGN)
        return pltpu.make_async_copy(rows_ref.at[pl.ds(first, size), :], out_refs[k].at[pl.ds(0, size), :], out_sem.at[k])

    for k in range(pieces):
        @pl.when(place[1, k] > 0)
        def _():
            store(k).start()
    for k in range(pieces):
        @pl.when(place[1, k] > 0)
        def _():
            store(k).wait()


def unpack(place, packed, pieces, capacity):
    d_model = packed.shape[1]
    return pl.pallas_call(
        functools.partial(unpack_kernel, pieces),
        out_shape=[jax.ShapeDtypeStruct((capacity, d_model), packed.dtype)] * pieces,
        in_specs=[pl.BlockSpec(memory_space=pltpu.SMEM), ANY],
        out_specs=[ANY] * pieces,
        scratch_shapes=[pltpu.VMEM(packed.shape, packed.dtype), pltpu.SemaphoreType.DMA, pltpu.SemaphoreType.DMA((pieces,))],
        compiler_params=params(),
        cost_estimate=pl.CostEstimate(flops=10**9, bytes_accessed=16 * 2**20, transcendentals=0),
        name='unpack',
    )(place, packed)


def expert_kernel(shards, d_model, width, first_col, first, carry, info, *refs):
    refs = list(refs)
    tok_ref = refs.pop(0)
    w_refs = [refs.pop(0) for _ in range(shards)]
    dx_in, dg_in = (None, None) if first else (refs.pop(0), refs.pop(0))
    old_refs = [refs.pop(0) for _ in range(shards)] if carry else []
    dx_out, dg_out = refs.pop(0), refs.pop(0)
    grad_refs = [refs.pop(0) for _ in range(shards)]
    w_mem, grads, x_t, g_t, dx_sum, w_sem, grad_sem = refs
    d_shard = d_model // shards
    step = pl.program_id(0)
    tiles, total, my_shard = info[0], info[1], info[2]

    def shard_rows(k):
        return pl.ds(pl.multiple_of((my_shard ^ k) * d_shard, ALIGN), d_shard)

    w_copies = [pltpu.make_async_copy(w_refs[k].at[:, :, pl.ds(first_col, width)], w_mem.at[:, shard_rows(k), :], w_sem.at[k]) for k in range(shards)]
    old_copies = [pltpu.make_async_copy(r, grads.at[:, shard_rows(k), :], grad_sem.at[k]) for k, r in enumerate(old_refs)]
    new_copies = [pltpu.make_async_copy(grads.at[:, shard_rows(k), :], r, grad_sem.at[k]) for k, r in enumerate(grad_refs)]

    @pl.when(step == 0)
    def _():
        for copy in w_copies + old_copies:
            copy.start()
        if not carry:
            grads[...] = jnp.zeros_like(grads)
        for copy in w_copies + old_copies:
            copy.wait()

    @pl.when(step < tiles)
    def _():
        row = step * TILE + lax.broadcasted_iota(I32, (TILE, 1), 0)
        tok = jnp.where(row < total, tok_ref[...].astype(F32), 0.0).astype(BF16)
        x, dy, g = tok[:, :d_model], tok[:, d_model:2 * d_model], tok[:, 2 * d_model:]
        x_t[...] = x.T
        g_t[...] = g.T
        dx_sum[...] = jnp.zeros_like(dx_sum) if first else dx_in[...]

        def chunk(c, dg):
            cols = pl.ds(pl.multiple_of(c * CHUNK, CHUNK), CHUNK)
            w_a, w_b, w_c = w_mem[0, :, cols], w_mem[1, :, cols], w_mem[2, :, cols]
            h_one = matmul(x, w_a)
            h_three = matmul(x, w_c)
            y_part = matmul(dy, w_b)
            d_act = matmul(g, w_b)
            sigma = jax.nn.sigmoid(h_one)
            silu = h_one * sigma
            act = (silu * h_three).astype(BF16)
            prod = act.astype(F32) * y_part
            dh_three = (d_act * silu).astype(BF16)
            dh_one = (d_act * h_three * sigma * (1.0 + h_one * (1.0 - sigma))).astype(BF16)
            grads[0, :, cols] += matmul(x_t[...], dh_one)
            grads[1, :, cols] += matmul(g_t[...], act)
            grads[2, :, cols] += matmul(x_t[...], dh_three)
            dx_sum[...] += matmul_nt(dh_one, w_a) + matmul_nt(dh_three, w_c)
            for j in range(CHUNK // LANES):
                dg = dg + prod[:, j * LANES:(j + 1) * LANES]
            return dg

        dg_out[...] = lax.fori_loop(0, width // CHUNK, chunk, jnp.zeros((TILE, LANES), F32) if first else dg_in[...])
        dx_out[...] = dx_sum[...].astype(dx_out.dtype)

    @pl.when(step == pl.num_programs(0) - 1)
    def _():
        for copy in new_copies:
            copy.start()
        for copy in new_copies:
            copy.wait()


def expert_block(info, tok, w_pieces, first_col, width, partial, old, last):
    rows, d_model = tok.shape[0], tok.shape[1] // 3
    shards = len(w_pieces)
    d_shard = d_model // shards
    first, carry = partial is None, old is not None
    row_block = lambda i, info: (jnp.minimum(i, jnp.maximum(info[0] - 1, 0)), 0)
    dx_spec, dg_spec = pl.BlockSpec((TILE, d_model), row_block), pl.BlockSpec((TILE, LANES), row_block)
    ins = [tok] + list(w_pieces) + ([] if first else list(partial)) + (list(old) if carry else [])
    in_specs = [pl.BlockSpec((TILE, 3 * d_model), row_block)] + [ANY] * shards + ([] if first else [dx_spec, dg_spec]) + ([ANY] * shards if carry else [])
    grad_shape = jax.ShapeDtypeStruct((3, d_shard, width), F32)
    dx_type = BF16 if last else F32
    aliases = {}
    if not first:
        aliases[1 + 1 + shards + 1] = 1
        if not last:
            aliases[1 + 1 + shards] = 0
    outs = pl.pallas_call(
        functools.partial(expert_kernel, shards, d_model, width, first_col, first, carry),
        out_shape=[jax.ShapeDtypeStruct((rows, d_model), dx_type), jax.ShapeDtypeStruct((rows, LANES), F32)] + [grad_shape] * shards,
        grid_spec=pltpu.PrefetchScalarGridSpec(
            num_scalar_prefetch=1,
            grid=(rows // TILE,),
            in_specs=in_specs,
            out_specs=[dx_spec, dg_spec] + [ANY] * shards,
            scratch_shapes=[
                pltpu.VMEM((3, d_model, width), BF16),
                pltpu.VMEM((3, d_model, width), F32),
                pltpu.VMEM((d_model, TILE), BF16),
                pltpu.VMEM((d_model, TILE), BF16),
                pltpu.VMEM((TILE, d_model), F32),
                pltpu.SemaphoreType.DMA((shards,)),
                pltpu.SemaphoreType.DMA((shards,)),
            ],
        ),
        input_output_aliases=aliases,
        compiler_params=params(),
        cost_estimate=pl.CostEstimate(flops=18 * (rows * 6 // 10) * d_model * width, bytes_accessed=40 * 2**20, transcendentals=rows * width),
        name='expert',
    )(info, *ins)
    return outs[:2], outs[2:]


def assemble_kernel(shards, first_col, width, fresh, info, *refs):
    piece_refs = refs[:shards]
    out_refs = refs[shards + (0 if fresh else 3):][:3]
    mem, in_sem, out_sem = refs[-3:]
    my_shard = info[0]
    loads = [pltpu.make_async_copy(piece_refs[k], mem.at[k], in_sem.at[k]) for k in range(shards)]
    stores = [[pltpu.make_async_copy(mem.at[k, j], out_refs[j].at[my_shard ^ k, :, pl.ds(first_col, width)], out_sem.at[k, j]) for j in range(3)] for k in range(shards)]
    for load in loads:
        load.start()
    for k in range(shards):
        loads[k].wait()
        for store in stores[k]:
            store.start()
    for k in range(shards):
        for store in stores[k]:
            store.wait()


def assemble(info, pieces, first_col, width, ff_dim, outs):
    shards = len(pieces)
    d_shard = pieces[0].shape[1]
    fresh = outs is None
    return pl.pallas_call(
        functools.partial(assemble_kernel, shards, first_col, width, fresh),
        out_shape=[jax.ShapeDtypeStruct((shards, d_shard, ff_dim), F32)] * 3,
        in_specs=[pl.BlockSpec(memory_space=pltpu.SMEM)] + [ANY] * (shards + (0 if fresh else 3)),
        out_specs=[ANY] * 3,
        scratch_shapes=[pltpu.VMEM((shards, 3, d_shard, width), F32), pltpu.SemaphoreType.DMA((shards,)), pltpu.SemaphoreType.DMA((shards, 3))],
        input_output_aliases={} if fresh else {1 + shards + j: j for j in range(3)},
        compiler_params=params(),
        cost_estimate=pl.CostEstimate(flops=10**9, bytes_accessed=20 * 2**20, transcendentals=0),
        name='assemble',
    )(info, *pieces, *([] if fresh else outs))


def solution(mesh):
    shards, ep_size = mesh.shape['fsdp'], mesh.shape['ep']
    devices = shards * ep_size
    tok_spec = P(None, BOTH, None)
    spec_edf = P('ep', 'fsdp', None)
    spec_efd = P('ep', None, 'fsdp')

    def local_step(x_in, dy_out, expert_idx, gate_prob, w_one, w_two, w_three):
        micro, tok_rows, d_model = x_in.shape
        top_k = expert_idx.shape[2]
        local_experts, d_shard, ff_dim = w_one.shape
        assert local_experts == shards
        capacity = capacity_of(tok_rows, top_k, devices)
        n_choice = tok_rows * top_k
        slots = devices * capacity
        blk, half = ff_dim // BLOCKS, ff_dim // HALVES
        my_shard = lax.axis_index('fsdp')
        me = my_shard * ep_size + lax.axis_index('ep')
        shard_info = my_shard.astype(I32)[None]

        w_all = [w_one, jnp.swapaxes(w_two, 1, 2), w_three]

        def send_half(h):
            pieces = []
            for k in range(shards):
                cut = [lax.dynamic_slice(w, (my_shard ^ k, 0, h * half), (1, d_shard, half))[0] for w in w_all]
                pieces.append(swap(jnp.stack(cut), 'fsdp', k, shards))
            return pieces

        w_halves = [send_half(0)]

        ids = expert_idx.reshape(micro, n_choice)
        dest = ((ids % local_experts) * ep_size + ids // local_experts) ^ me
        one_hot = (dest[:, None, :] == jnp.arange(devices, dtype=I32)[None, :, None]).astype(I32)
        running = jnp.cumsum(one_hot, axis=2)
        position = jnp.sum((running - one_hot) * one_hot, axis=1)
        kept = jnp.minimum(running[:, :, -1], capacity)
        choice_slot = jnp.where(position < capacity, dest * capacity + position, slots)

        zero_row = jnp.zeros((1, 2 * d_model), x_in.dtype)
        sent_tok, sent_gate = [], []
        for m in range(micro):
            holder = jnp.full((slots + 1,), n_choice, I32).at[choice_slot[m]].set(jnp.arange(n_choice, dtype=I32))[:slots]
            table = jnp.concatenate([jnp.concatenate([x_in[m], dy_out[m]], axis=1), zero_row], axis=0)
            tok_slot = (holder // top_k).reshape(devices, capacity)
            sent_tok.append([swap(table[tok_slot[k]], BOTH, k, devices) for k in range(devices)])
            gate_pad = jnp.concatenate([gate_prob[m].reshape(n_choice), jnp.zeros((1,), F32)])
            gate_slot = gate_pad[holder].reshape(devices, capacity)
            gate_slot = jnp.concatenate([gate_slot, jnp.broadcast_to(kept[m].astype(F32)[:, None], (devices, LANES))], axis=1)
            sent_gate.append(jnp.stack([swap(gate_slot[k], BOTH, k, devices) for k in range(devices)]))
        w_halves.append(send_half(1))

        dx_parts, dg_parts = [], []
        grads = [None] * BLOCKS
        outs = None
        for m in range(micro):
            gates = sent_gate[m]
            counts = gates[:, capacity].astype(I32)
            sizes = (counts + ALIGN - 1) // ALIGN * ALIGN
            starts = jnp.cumsum(sizes) - sizes
            place = jnp.stack([starts, sizes])
            total = jnp.sum(sizes)
            info = jnp.stack([(total + TILE - 1) // TILE, total, my_shard.astype(I32)])
            gate_wide = jnp.broadcast_to(gates[:, :capacity, None], (devices, capacity, LANES))
            tok = pack(place, sent_tok[m], gate_wide, capacity, d_model)
            partial = None
            for b in range(BLOCKS):
                h, col = b * blk // half, b * blk % half
                partial, grads[b] = expert_block(info, tok, w_halves[h], col, blk, partial, grads[b], b == BLOCKS - 1)
            back = unpack(place, partial[0], devices, capacity)
            back = jnp.concatenate([swap(v, BOTH, k, devices) for k, v in enumerate(back)] + [zero_row[:, :d_model]])
            dg_rows = jnp.concatenate([jnp.sum(partial[1], axis=1), jnp.zeros((capacity,), F32)])
            dg_back = [swap(lax.dynamic_slice(dg_rows, (starts[k],), (capacity,)), BOTH, k, devices) for k in range(devices)]
            dg_back = jnp.concatenate(dg_back + [jnp.zeros((1,), F32)])
            slot = choice_slot[m].reshape(tok_rows, top_k)
            total_dx = sum(back[slot[:, j]].astype(F32) for j in range(top_k))
            dx_parts.append(total_dx.astype(BF16))
            dg_parts.append(dg_back[choice_slot[m]].reshape(tok_rows, top_k))
        for b in range(BLOCKS):
            moved = [swap(v, 'fsdp', k, shards) for k, v in enumerate(grads[b])]
            outs = assemble(shard_info, moved, b * blk, blk, ff_dim, outs)
        dw_one, dw_two, dw_three = outs
        return jnp.stack(dx_parts), jnp.stack(dg_parts), dw_one, jnp.swapaxes(dw_two, 1, 2), dw_three

    return jax.shard_map(local_step, mesh=mesh, in_specs=(tok_spec, tok_spec, tok_spec, tok_spec, spec_edf, spec_efd, spec_edf), out_specs=(tok_spec, tok_spec, spec_edf, spec_efd, spec_edf), check_vma=False)
```

```python
import functools

import jax
import jax.numpy as jnp
from jax import lax
from jax.experimental import pallas as pl
from jax.experimental.pallas import tpu as pltpu
from jax.sharding import PartitionSpec as P


BLOCKS = 4
TILE = 512
CHUNK = 256
ALIGN = 16
LANES = 128
BF16 = jnp.bfloat16
F32 = jnp.float32
I32 = jnp.int32
BOTH = ('fsdp', 'ep')
ANY = pl.BlockSpec(memory_space=pl.ANY)


def capacity_of(tok_rows, top_k, experts):
    return 8 * ((5 * tok_rows * top_k + 32 * experts - 1) // (32 * experts))


def swap(value, axes, shift, devices):
    if shift == 0:
        return value
    return lax.ppermute(value, axes, [(s, s ^ shift) for s in range(devices)])


def matmul(left, right):
    return jnp.dot(left, right, preferred_element_type=F32)


def matmul_nt(left, right):
    return lax.dot_general(left, right, (((1,), (1,)), ((), ())), preferred_element_type=F32)


def params():
    return pltpu.CompilerParams(vmem_limit_bytes=60 * 2**20)


def dispatch_kernel(pieces, local_experts, ep_size, capacity, micro_index, info, ids_ref, gate_ref, x_hbm, dy_hbm, *refs):
    out_refs, gates_out, slot_out = refs[:pieces], refs[pieces], refs[pieces + 1]
    table, held, held_gate, rows, table_sem, row_sem = refs[pieces + 2:]
    tokens, d_model = x_hbm.shape[1:]
    copies = [pltpu.make_async_copy(r.at[micro_index], table.at[:, pl.ds(j * d_model, d_model)], table_sem.at[j]) for j, r in enumerate((x_hbm, dy_hbm))]
    for copy in copies:
        copy.start()

    ids = ids_ref[...]
    dest = ((ids % local_experts) * ep_size + ids // local_experts) ^ info[0]
    piece = lax.broadcasted_iota(I32, (pieces, tokens), 0)
    lane = lax.broadcasted_iota(I32, (pieces, tokens), 1)
    first, second = dest[0:1] == piece, dest[1:2] == piece
    member = (first | second).astype(I32)
    running = member
    step = 1
    while step < tokens:
        running = running + jnp.where(lane >= step, pltpu.roll(running, step, 1), 0)
        step *= 2
    position = running - member
    kept = position < capacity
    held[...] = jnp.where((first | second) & kept, position, -1)
    held_gate[...] = jnp.where(first, gate_ref[0:1], gate_ref[1:2])
    slot = jnp.where(kept, piece * capacity + position, pieces * capacity)
    slot_out[0:1, :] = jnp.sum(jnp.where(first, slot, 0), axis=0, keepdims=True)
    slot_out[1:2, :] = jnp.sum(jnp.where(second, slot, 0), axis=0, keepdims=True)
    count = jnp.minimum(jnp.max(running, axis=1, keepdims=True), capacity)
    gates_out[:, pl.ds(capacity, LANES)] = jnp.broadcast_to(count.astype(F32), (pieces, LANES))
    for copy in copies:
        copy.wait()

    part = capacity // 2

    def store(k, ref):
        return pltpu.make_async_copy(rows.at[k % 2], ref, row_sem.at[k % 2])

    def one_piece(k, carry):
        @pl.when(k >= 2)
        def _():
            store(k, out_refs[0]).wait()

        wanted = held[pl.ds(k, 1), :]
        gate_row = held_gate[pl.ds(k, 1), :]
        for h in range(2):
            def half():
                place = h * part + lax.broadcasted_iota(I32, (part, LANES), 0)
                total = jnp.zeros((part, LANES), F32)
                chosen = []
                for c in range(tokens // LANES):
                    cols = slice(c * LANES, (c + 1) * LANES)
                    hit = place == wanted[:, cols]
                    total = total + jnp.where(hit, gate_row[:, cols], 0.0)
                    chosen.append(jnp.where(hit, 1.0, 0.0).astype(BF16))
                picked = matmul(jnp.concatenate(chosen, axis=1), table[...])
                rows[k % 2, pl.ds(h * part, part), :] = picked.astype(BF16)
                held_gate_row = jnp.sum(total.T, axis=0, keepdims=True)
                return held_gate_row

            used = jnp.max(wanted) >= h * part
            if h == 0:
                low = half()
            else:
                high = lax.cond(used, half, lambda: jnp.zeros((1, part), F32))
        gates_out[pl.ds(k, 1), pl.ds(0, capacity)] = jnp.concatenate([low, high], axis=1)
        for j in range(pieces):
            @pl.when(k == j)
            def _():
                store(k, out_refs[j]).start()
        return carry

    lax.fori_loop(0, pieces, one_piece, 0)
    for k in range(pieces - 2, pieces):
        store(k, out_refs[0]).wait()


def dispatch(info, ids, gates, x_in, dy_out, micro_index, pieces, local_experts, ep_size, capacity):
    tokens, d_model = x_in.shape[1:]
    vmem = pl.BlockSpec(memory_space=pltpu.VMEM)
    outs = pl.pallas_call(
        functools.partial(dispatch_kernel, pieces, local_experts, ep_size, capacity, micro_index),
        out_shape=[jax.ShapeDtypeStruct((capacity, 2 * d_model), BF16)] * pieces + [jax.ShapeDtypeStruct((pieces, capacity + LANES), F32), jax.ShapeDtypeStruct(ids.shape, I32)],
        in_specs=[pl.BlockSpec(memory_space=pltpu.SMEM), vmem, vmem, ANY, ANY],
        out_specs=[ANY] * pieces + [vmem, vmem],
        scratch_shapes=[
            pltpu.VMEM((tokens, 2 * d_model), BF16),
            pltpu.VMEM((pieces, tokens), I32),
            pltpu.VMEM((pieces, tokens), F32),
            pltpu.VMEM((2, capacity, 2 * d_model), BF16),
            pltpu.SemaphoreType.DMA((2,)),
            pltpu.SemaphoreType.DMA((2,)),
        ],
        compiler_params=params(),
        cost_estimate=pl.CostEstimate(flops=2 * pieces * capacity * tokens * 2 * d_model, bytes_accessed=24 * 2**20, transcendentals=0),
        name='dispatch',
    )(info, ids, gates, x_in, dy_out)
    return outs[:pieces], outs[pieces], outs[pieces + 1]


def pack_kernel(pieces, d_model, counts, *refs):
    tok_refs, gates_ref, out_ref, place = refs[:pieces], refs[pieces], refs[pieces + 1], refs[pieces + 2]
    tok, gates, gated, blank, in_sem, gate_sem, out_sem, blank_sem = refs[pieces + 3:]
    gate_copy = pltpu.make_async_copy(gates_ref, gates, gate_sem)
    gate_copy.start()
    loads = [pltpu.make_async_copy(tok_refs[k], tok.at[k], in_sem.at[k]) for k in range(pieces)]
    for load in loads:
        load.start()
    total = jnp.int32(0)
    for k in range(pieces):
        size = (counts[k] + ALIGN - 1) // ALIGN * ALIGN
        place[0, k], place[1, k] = total, size
        total = total + size
    tiles = (total + TILE - 1) // TILE
    place[2, 0], place[2, 1] = tiles, total
    rest = tiles * TILE - total
    blank[...] = jnp.zeros_like(blank)

    def blank_copy():
        size = pl.multiple_of(rest, ALIGN)
        return pltpu.make_async_copy(blank.at[pl.ds(0, size), :], out_ref.at[pl.ds(pl.multiple_of(total, ALIGN), size), :], blank_sem)

    @pl.when(rest > 0)
    def _():
        blank_copy().start()

    gate_copy.wait()

    def stores(k):
        first = pl.multiple_of(place[0, k], ALIGN)
        size = pl.multiple_of(place[1, k], ALIGN)
        used, rows = pl.ds(0, size), pl.ds(first, size)
        return [
            pltpu.make_async_copy(tok.at[k, used, :], out_ref.at[rows, pl.ds(0, 2 * d_model)], out_sem.at[k, 0]),
            pltpu.make_async_copy(gated.at[k, used, :], out_ref.at[rows, pl.ds(2 * d_model, d_model)], out_sem.at[k, 1]),
        ]

    for k in range(pieces):
        loads[k].wait()

        @pl.when(place[1, k] > 0)
        def _():
            def gate_rows(r, carry):
                rows = pl.ds(pl.multiple_of(r * LANES, LANES), LANES)
                for c in range(d_model // LANES):
                    dy = tok[k, rows, pl.ds(d_model + c * LANES, LANES)].astype(F32)
                    gated[k, rows, pl.ds(c * LANES, LANES)] = (gates[k, rows, :] * dy).astype(BF16)
                return carry

            lax.fori_loop(0, (place[1, k] + LANES - 1) // LANES, gate_rows, 0)
            for store in stores(k):
                store.start()

    for k in range(pieces):
        @pl.when(place[1, k] > 0)
        def _():
            for store in stores(k):
                store.wait()

    @pl.when(rest > 0)
    def _():
        blank_copy().wait()


def pack(counts, tokens, gates, capacity, d_model):
    pieces = len(tokens)
    smem = pl.BlockSpec(memory_space=pltpu.SMEM)
    return pl.pallas_call(
        functools.partial(pack_kernel, pieces, d_model),
        out_shape=[jax.ShapeDtypeStruct((pieces * capacity, 3 * d_model), BF16), jax.ShapeDtypeStruct((3, pieces), I32)],
        in_specs=[smem] + [ANY] * (pieces + 1),
        out_specs=[ANY, smem],
        scratch_shapes=[
            pltpu.VMEM((pieces, capacity, 2 * d_model), BF16),
            pltpu.VMEM((pieces, capacity, LANES), F32),
            pltpu.VMEM((pieces, capacity, d_model), BF16),
            pltpu.VMEM((TILE, 3 * d_model), BF16),
            pltpu.SemaphoreType.DMA((pieces,)),
            pltpu.SemaphoreType.DMA,
            pltpu.SemaphoreType.DMA((pieces, 2)),
            pltpu.SemaphoreType.DMA,
        ],
        compiler_params=params(),
        cost_estimate=pl.CostEstimate(flops=10**9, bytes_accessed=40 * 2**20, transcendentals=0),
        name='pack',
    )(counts, *tokens, gates)


def unpack_kernel(pieces, place, packed_ref, *refs):
    out_refs = refs[:pieces]
    rows_ref, in_sem, out_sem = refs[pieces:]
    load = pltpu.make_async_copy(packed_ref, rows_ref, in_sem)
    load.start()
    load.wait()

    def store(k):
        first = pl.multiple_of(place[0, k], ALIGN)
        size = pl.multiple_of(place[1, k], ALIGN)
        return pltpu.make_async_copy(rows_ref.at[pl.ds(first, size), :], out_refs[k].at[pl.ds(0, size), :], out_sem.at[k])

    for k in range(pieces):
        @pl.when(place[1, k] > 0)
        def _():
            store(k).start()
    for k in range(pieces):
        @pl.when(place[1, k] > 0)
        def _():
            store(k).wait()


def unpack(place, packed, pieces, capacity):
    d_model = packed.shape[1]
    return pl.pallas_call(
        functools.partial(unpack_kernel, pieces),
        out_shape=[jax.ShapeDtypeStruct((capacity, d_model), packed.dtype)] * pieces,
        in_specs=[pl.BlockSpec(memory_space=pltpu.SMEM), ANY],
        out_specs=[ANY] * pieces,
        scratch_shapes=[pltpu.VMEM(packed.shape, packed.dtype), pltpu.SemaphoreType.DMA, pltpu.SemaphoreType.DMA((pieces,))],
        compiler_params=params(),
        cost_estimate=pl.CostEstimate(flops=10**9, bytes_accessed=16 * 2**20, transcendentals=0),
        name='unpack',
    )(place, packed)


def expert_kernel(shards, d_model, width, first, last, carry, place, info, *refs):
    refs = list(refs)
    tok_ref = refs.pop(0)
    w_refs = [refs.pop(0) for _ in range(shards)]
    dx_in, dg_in, flip = (None, None, None) if first else (refs.pop(0), refs.pop(0), refs.pop(0))
    old_refs = [refs.pop(0) for _ in range(shards)] if carry else []
    dx_out, dg_out = refs.pop(0), refs.pop(0)
    if first:
        flip = refs.pop(0)
    grad_refs = [refs.pop(0) for _ in range(shards)]
    w_mem, grads, dx_sum, w_sem, old_sem, new_sem = refs
    d_shard = d_model // shards
    step = pl.program_id(0)
    tiles, my_shard = place[2, 0], info[0]
    chunks = width // CHUNK

    def shard_rows(k):
        return pl.ds(pl.multiple_of((my_shard ^ k) * d_shard, ALIGN), d_shard)

    def cols_of(c):
        return pl.ds(c * CHUNK if isinstance(c, int) else pl.multiple_of(c * CHUNK, CHUNK), CHUNK)

    def loads(c):
        found = [pltpu.make_async_copy(w_refs[k].at[:, :, cols_of(c)], w_mem.at[:, shard_rows(k), cols_of(c)], w_sem.at[k, c]) for k in range(shards)]
        return found + [pltpu.make_async_copy(r.at[:, :, cols_of(c)], grads.at[:, shard_rows(k), cols_of(c)], old_sem.at[k, c]) for k, r in enumerate(old_refs)]

    def stores(c):
        return [pltpu.make_async_copy(grads.at[:, shard_rows(k), cols_of(c)], r.at[:, :, cols_of(c)], new_sem.at[k, c]) for k, r in enumerate(grad_refs)]

    @pl.when(step == 0)
    def _():
        for c in range(chunks):
            for copy in loads(c):
                copy.start()
        if not carry:
            grads[...] = jnp.zeros_like(grads)

    @pl.when(step < tiles)
    def _():
        if first:
            flip[0, 0] = tok_ref[:, pl.ds(0, d_model)].T
            flip[0, 1] = tok_ref[:, pl.ds(2 * d_model, d_model)].T
        dx_sum[...] = jnp.zeros_like(dx_sum) if first else dx_in[...]

        def chunk(c, dg):
            @pl.when(step == 0)
            def _():
                for copy in loads(c):
                    copy.wait()

            cols = cols_of(c)
            x, dy, g = (tok_ref[:, pl.ds(j * d_model, d_model)] for j in range(3))
            w_a, w_b, w_c = w_mem[0, :, cols], w_mem[1, :, cols], w_mem[2, :, cols]
            h_one = matmul(x, w_a)
            h_three = matmul(x, w_c)
            y_part = matmul(dy, w_b)
            d_act = matmul(g, w_b)
            sigma = jax.nn.sigmoid(h_one)
            silu = h_one * sigma
            act = (silu * h_three).astype(BF16)
            prod = act.astype(F32) * y_part
            dh_three = (d_act * silu).astype(BF16)
            dh_one = (d_act * h_three * sigma * (1.0 + h_one * (1.0 - sigma))).astype(BF16)
            grads[0, :, cols] += matmul(flip[0, 0], dh_one)
            grads[1, :, cols] += matmul(flip[0, 1], act)
            grads[2, :, cols] += matmul(flip[0, 0], dh_three)
            dx_sum[...] += matmul_nt(dh_one, w_a) + matmul_nt(dh_three, w_c)
            for j in range(CHUNK // LANES):
                dg = dg + prod[:, j * LANES:(j + 1) * LANES]

            @pl.when(step == tiles - 1)
            def _():
                for copy in stores(c):
                    copy.start()

            return dg

        dg = lax.fori_loop(0, chunks, chunk, jnp.zeros((TILE, LANES), F32) if first else dg_in[...])
        dx_out[...] = dx_sum[...].astype(dx_out.dtype)
        if last:
            dg_out[0] = jnp.broadcast_to(jnp.sum(dg.T, axis=0, keepdims=True), (8, TILE))
        else:
            dg_out[...] = dg

    @pl.when((step == 0) & (tiles == 0))
    def _():
        for c in range(chunks):
            for copy in loads(c):
                copy.wait()
        for c in range(chunks):
            for copy in stores(c):
                copy.start()

    @pl.when(step == pl.num_programs(0) - 1)
    def _():
        for c in range(chunks):
            for copy in stores(c):
                copy.wait()


def expert_block(place, info, tok, w_pieces, partial, old, last):
    rows, d_model = tok.shape[0], tok.shape[1] // 3
    shards = len(w_pieces)
    d_shard, width = w_pieces[0].shape[1:]
    first, carry = partial is None, old is not None
    at = lambda i, place: jnp.minimum(i, jnp.maximum(place[2, 0] - 1, 0))
    row_block = lambda i, place, info: (at(i, place), 0)
    dx_spec, dg_spec = pl.BlockSpec((TILE, d_model), row_block), pl.BlockSpec((TILE, LANES), row_block)
    flip_spec = pl.BlockSpec((1, 2, d_model, TILE), lambda i, place, info: (at(i, place), 0, 0, 0))
    flip_shape = jax.ShapeDtypeStruct((rows // TILE, 2, d_model, TILE), BF16)
    ins = [tok] + list(w_pieces) + ([] if first else list(partial)) + (list(old) if carry else [])
    in_specs = [pl.BlockSpec((TILE, 3 * d_model), row_block)] + [ANY] * shards + ([] if first else [dx_spec, dg_spec, flip_spec]) + ([ANY] * shards if carry else [])
    out_shape = [jax.ShapeDtypeStruct((rows, d_model), BF16 if last else F32)]
    out_specs = [dx_spec]
    if last:
        out_shape.append(jax.ShapeDtypeStruct((rows // TILE, 8, TILE), F32))
        out_specs.append(pl.BlockSpec((1, 8, TILE), lambda i, place, info: (at(i, place), 0, 0)))
    else:
        out_shape.append(jax.ShapeDtypeStruct((rows, LANES), F32))
        out_specs.append(dg_spec)
    if first:
        out_shape.append(flip_shape)
        out_specs.append(flip_spec)
    head = len(out_shape)
    aliases = {} if first or last else {2 + 1 + shards: 0, 2 + 1 + shards + 1: 1}
    outs = pl.pallas_call(
        functools.partial(expert_kernel, shards, d_model, width, first, last, carry),
        out_shape=out_shape + [jax.ShapeDtypeStruct((3, d_shard, width), F32)] * shards,
        grid_spec=pltpu.PrefetchScalarGridSpec(
            num_scalar_prefetch=2,
            grid=(rows // TILE,),
            in_specs=in_specs,
            out_specs=out_specs + [ANY] * shards,
            scratch_shapes=[
                pltpu.VMEM((3, d_model, width), BF16),
                pltpu.VMEM((3, d_model, width), F32),
                pltpu.VMEM((TILE, d_model), F32),
                pltpu.SemaphoreType.DMA((shards, width // CHUNK)),
                pltpu.SemaphoreType.DMA((shards, width // CHUNK)),
                pltpu.SemaphoreType.DMA((shards, width // CHUNK)),
            ],
        ),
        input_output_aliases=aliases,
        compiler_params=params(),
        cost_estimate=pl.CostEstimate(flops=18 * (rows * 6 // 10) * d_model * width, bytes_accessed=40 * 2**20, transcendentals=rows * width),
        name='expert',
    )(place, info, *ins)
    flip = outs[2] if first else partial[2]
    return (outs[0], outs[1], flip), outs[head:]


def assemble_kernel(shards, first_col, width, fresh, info, *refs):
    piece_refs = refs[:shards]
    out_refs = refs[shards + (0 if fresh else 3):][:3]
    mem, in_sem, out_sem = refs[-3:]
    my_shard = info[0]
    loads = [pltpu.make_async_copy(piece_refs[k], mem.at[k], in_sem.at[k]) for k in range(shards)]
    stores = [[pltpu.make_async_copy(mem.at[k, j], out_refs[j].at[my_shard ^ k, :, pl.ds(first_col, width)], out_sem.at[k, j]) for j in range(3)] for k in range(shards)]
    for load in loads:
        load.start()
    for k in range(shards):
        loads[k].wait()
        for store in stores[k]:
            store.start()
    for k in range(shards):
        for store in stores[k]:
            store.wait()


def assemble(info, pieces, first_col, width, ff_dim, outs):
    shards = len(pieces)
    d_shard = pieces[0].shape[1]
    fresh = outs is None
    return pl.pallas_call(
        functools.partial(assemble_kernel, shards, first_col, width, fresh),
        out_shape=[jax.ShapeDtypeStruct((shards, d_shard, ff_dim), F32)] * 3,
        in_specs=[pl.BlockSpec(memory_space=pltpu.SMEM)] + [ANY] * (shards + (0 if fresh else 3)),
        out_specs=[ANY] * 3,
        scratch_shapes=[pltpu.VMEM((shards, 3, d_shard, width), F32), pltpu.SemaphoreType.DMA((shards,)), pltpu.SemaphoreType.DMA((shards, 3))],
        input_output_aliases={} if fresh else {1 + shards + j: j for j in range(3)},
        compiler_params=params(),
        cost_estimate=pl.CostEstimate(flops=10**9, bytes_accessed=20 * 2**20, transcendentals=0),
        name='assemble',
    )(info, *pieces, *([] if fresh else outs))


def solution(mesh):
    shards, ep_size = mesh.shape['fsdp'], mesh.shape['ep']
    devices = shards * ep_size
    tok_spec = P(None, BOTH, None)
    spec_edf = P('ep', 'fsdp', None)
    spec_efd = P('ep', None, 'fsdp')

    def local_step(x_in, dy_out, expert_idx, gate_prob, w_one, w_two, w_three):
        micro, tok_rows, d_model = x_in.shape
        top_k = expert_idx.shape[2]
        local_experts, d_shard, ff_dim = w_one.shape
        assert local_experts == shards
        capacity = capacity_of(tok_rows, top_k, devices)
        slots = devices * capacity
        blk = ff_dim // BLOCKS
        my_shard = lax.axis_index('fsdp').astype(I32)
        me = my_shard * ep_size + lax.axis_index('ep').astype(I32)
        shard_info, device_info = my_shard[None], me[None]

        w_all = [w_one, jnp.swapaxes(w_two, 1, 2), w_three]

        def send_weights(b):
            pieces = []
            for k in range(shards):
                cut = [lax.dynamic_slice(w, (my_shard ^ k, 0, b * blk), (1, d_shard, blk))[0] for w in w_all]
                pieces.append(swap(jnp.stack(cut), 'fsdp', k, shards))
            return pieces

        w_blocks = [send_weights(b) for b in range(BLOCKS)]

        ids = jnp.transpose(expert_idx, (0, 2, 1))
        gate_rows = jnp.transpose(gate_prob, (0, 2, 1))
        sent_tok, sent_gate, slots_of = [], [], []
        for m in range(micro):
            rows, gates, slot = dispatch(device_info, ids[m], gate_rows[m], x_in, dy_out, m, devices, local_experts, ep_size, capacity)
            slots_of.append(slot)
            sent_gate.append(jnp.stack([swap(gates[k], BOTH, k, devices) for k in range(devices)]))
            sent_tok.append([swap(rows[k], BOTH, k, devices) for k in range(devices)])

        zero_row = jnp.zeros((1, d_model), BF16)
        dx_parts, dg_parts = [], []
        grads = [None] * BLOCKS
        outs = None
        for m in range(micro):
            gates = sent_gate[m]
            counts = gates[:, capacity].astype(I32)
            gate_wide = jnp.broadcast_to(gates[:, :capacity, None], (devices, capacity, LANES))
            tok, place = pack(counts, sent_tok[m], gate_wide, capacity, d_model)
            partial = None
            for b in range(BLOCKS):
                partial, grads[b] = expert_block(place, shard_info, tok, w_blocks[b], partial, grads[b], b == BLOCKS - 1)
            back = unpack(place, partial[0], devices, capacity)
            note = jnp.concatenate([partial[1][:, 0, :].reshape(-1), place[0].astype(F32), jnp.zeros((LANES - devices,), F32)])
            back = [swap(v, BOTH, k, devices) for k, v in enumerate(back)]
            notes = [swap(note, BOTH, k, devices) for k in range(devices)]
            back = jnp.concatenate(back + [zero_row])
            notes = jnp.stack(notes)
            slot = slots_of[m]
            total_dx = sum(back[slot[j]].astype(F32) for j in range(top_k))
            dx_parts.append(total_dx.astype(BF16))
            first_row = jnp.stack([notes[k, slots + k] for k in range(devices)]).astype(I32)
            shift = first_row + jnp.arange(devices, dtype=I32) * notes.shape[1]
            piece, position = slot // capacity, slot % capacity
            where_dg = position + jnp.sum(jnp.where(piece[..., None] == jnp.arange(devices), shift, 0), axis=-1)
            dg = jnp.where(piece < devices, notes.reshape(-1)[jnp.where(piece < devices, where_dg, 0)], 0.0)
            dg_parts.append(jnp.transpose(dg))
        for b in range(BLOCKS):
            moved = [swap(v, 'fsdp', k, shards) for k, v in enumerate(grads[b])]
            outs = assemble(shard_info, moved, b * blk, blk, ff_dim, outs)
        dw_one, dw_two, dw_three = outs
        return jnp.stack(dx_parts), jnp.stack(dg_parts), dw_one, jnp.swapaxes(dw_two, 1, 2), dw_three

    return jax.shard_map(local_step, mesh=mesh, in_specs=(tok_spec, tok_spec, tok_spec, tok_spec, spec_edf, spec_efd, spec_edf), out_specs=(tok_spec, tok_spec, spec_edf, spec_efd, spec_edf), check_vma=False)
```
